256 devices in a mesh: ga: 2 (over z), aa: 64 (over y, x), ba: 2 (over core).
Axes of the slice: x: 8, y: 8, z: 2, core: 2. Of those that a mesh axis runs over, the one named last changes fastest.
The devices are a block of a 8x8x16 slice.
Arguments:
- images: bfloat16 [16384, 12, 4096], P(('ga', 'aa', 'ba')), parts along dimension 0, may hold values from -6 to 6
- key_projection: bfloat16 [4096, 512], replicated, may hold values from -0.09375 to 0.09375
- value_projection: bfloat16 [4096, 512], replicated, may hold values from -0.09375 to 0.09375
- key_norm_gain: float32 [128], replicated, may hold values from 0.1 to 1.9
- hidden: bfloat16 [16384, 4096], P(('ga', 'aa'), 'ba'), parts along dimension 0, may hold values from -6 to 6
- shared_query_base: bfloat16 [16384, 2048], P(('ga', 'aa'), 'ba'), parts along dimension 0, may hold values from -220 to 220
- adapter_down_matrix: bfloat16 [64, 4096, 16], P('aa'), may hold values from -0.09375 to 0.09375
- adapter_up_matrix: bfloat16 [64, 16, 2048], P('aa'), may hold values from -1.5 to 1.5
- tenant_adapter_index: int32 [16384, 1], P(('ga', 'aa')), parts along dimension 0, may hold values from 0 to 63; in each aligned block of 128 rows (0 to 127, 128 to 255, ...) at most 4 rows name the same one
- used_tile_count: int32 [16384], P(('ga', 'aa', 'ba')), parts along dimension 0, may hold values from 1 to 4
Outputs:
- attended: bfloat16 [16384, 2048], P(('ga', 'aa', 'ba')), parts along dimension 0
The draws below stay inside these ranges and needn't reach their ends.
There are 2 independent parts, one for each index of `ga`. The reference program is written for one: setup_inputs(seed, part) draws one part's arguments, and reference() takes and returns one part's arrays. A program takes and returns all parts, laid end to end along the dimension named above; an argument that names none is the same for every part. Nothing has to cross between parts.
Inputs may be any that keep to these rules, and one draw needn't show every extreme that they name: `tenant_adapter_index`: among the 128 requests of one index of aa (aligned blocks) no adapter is named more than 4 times.
All inputs are finite; a program needn't handle non-finite values.
Results may differ from the reference program's by a relative error of at most 0.012.
The reference program's roundings to bfloat16 on the way count: a program that leaves them out, or rounds other values in their place, can miss the bound.
Values may be sent and summed in bfloat16 or wider, within the bound.
No kernel may reach another device: no remote copies, remote signals or barrier semaphores. Data moves between devices by JAX's collectives and lax.ppermute only.
A program may use at most 128 MiB of HBM per device.

```python
import math
import jax
import jax.numpy as jnp
import numpy as np
from jax import lax

MODEL_WIDTH = 4096
HEAD_WIDTH = 128
QUERY_HEADS = 16
KEY_VALUE_HEADS = 4
ADAPTER_RANK = 16
TILE_SLOTS = 4
TILE_TOKENS = 3
REQ_DEV = 128
REQUEST_TOTAL = 8192
ADAPTER_TOTAL = 64
MOST = 4
QUERY_WIDTH = 2048
KVW = 512


def draw_shared_query_base(key, part):
    key_values = jax.random.fold_in(jax.random.fold_in(key, 17), 0)
    normal_part = jnp.clip(jax.random.normal(key_values, (REQUEST_TOTAL, QUERY_WIDTH), jnp.float32), -6.0, 6.0)
    return normal_part.astype(jnp.bfloat16)


def place_ends(entries, own_key, smallest, largest):
    spot = [jax.random.randint(jax.random.fold_in(own_key, axis), (), 0, length) for axis, length in enumerate(entries.shape)]
    longest = entries.shape.index(max(entries.shape))
    next_to = spot[:longest] + [(spot[longest] + 1) % entries.shape[longest]] + spot[longest + 1:]
    return entries.at[tuple(spot)].set(smallest).at[tuple(next_to)].set(largest)


def level_of(own_key, extent, cuts, smallest, high):
    level = 1.0
    for dim, shards_of in cuts:
        steps = jax.random.uniform(jax.random.fold_in(jax.random.fold_in(own_key, 6), dim), (shards_of,), jnp.float32, smallest / len(cuts), high / len(cuts))
        level = level * jnp.repeat(jnp.exp(steps), extent[dim] // shards_of).reshape((-1,) + (1,) * (len(extent) - 1 - dim))
    return level


def assign_block(stream_key, own, number, rows, count, top, most, slope):
    order = jax.random.permutation(stream_key, count)
    heavy_load, common = shares(count, rows * top, most, slope, True), shares(count, rows * top, most, slope, False)
    places = jnp.arange(count)

    def named(sizes, offset_by):
        used = int((sizes > 0).sum())
        fixed = max(1, used // 4)
        passed = fixed + (places - fixed + offset_by * (used - fixed)) % max(1, count - fixed)
        return jnp.zeros((count,), jnp.int32).at[order[jnp.where(places < fixed, places, passed)]].set(jnp.asarray(sizes, jnp.int32))

    sizes = jnp.where(number % 4 == 0, named(heavy_load, number // 4), named(common, number - number // 4 - 1))
    mixed = jax.random.permutation(jax.random.fold_in(own, 3), count)
    donor, receiver = mixed[0:count // 2 * 2:2], mixed[1:count // 2 * 2:2]
    room = jnp.minimum(sizes[donor] - 1, most - sizes[receiver]) // 2
    room = jnp.where((donor == order[0]) | (receiver == order[0]) | (sizes[receiver] == 0), 0, jnp.maximum(room, 0))
    passed = jax.random.randint(jax.random.fold_in(own, 4), (count // 2,), 0, 1 << 20) % (room + 1)
    sizes = sizes.at[donor].add(-passed).at[receiver].add(passed)
    members = jnp.searchsorted(jnp.cumsum(sizes), jnp.arange(rows * top), side="right").astype(jnp.int32)
    table = members.reshape(top, rows).T
    table = table[jax.random.permutation(jax.random.fold_in(own, 1), rows)]
    offset_by = jax.random.randint(jax.random.fold_in(own, 2), (rows, 1), 0, top)
    return jnp.take_along_axis(table, (jnp.arange(top)[None, :] + offset_by) % top, axis=1)


def shares(amount, total, most, slope, full):
    weights = [(1 << 20) // math.isqrt(standing ** slope) + 1 for standing in range(1, amount + 1)]
    largest = most if full else min(most, max(-(-total // amount), total * weights[0] // sum(weights)))
    least = 1 if total - largest >= amount - 1 else 0
    holding, spare = [largest] + [least] * (amount - 1), total - largest - least * (amount - 1)
    while spare > 0:
        candidates = [i for i in range(1, amount) if holding[i] < largest] or [i for i in range(1, amount) if holding[i] < most]
        mass, remaining = sum([weights[i] for i in candidates]), spare
        for i in candidates:
            addition = min(most - holding[i], max(1, remaining * weights[i] // mass), spare)
            holding[i] = holding[i] + addition
            spare = spare - addition
    return np.array(holding)


def bell_draw(key, shape, spread, bound, pieces=(), kind=jnp.bfloat16):
    entries = spread * jax.random.normal(key, shape, jnp.float32)
    if pieces:
        entries = entries * level_of(key, shape, pieces, -0.22, 0.18)
    return jnp.clip(entries, -bound, bound).astype(kind)


def setup_inputs(seed: int = 0, part: int = 0) -> dict:
    keys = jax.random.split(jax.random.key(seed), 11)
    own_keys = jax.random.split(jax.random.fold_in(keys[10], part), 11)
    images = bell_draw(own_keys[0], (REQUEST_TOTAL, TILE_SLOTS * TILE_TOKENS, MODEL_WIDTH), 1.0, 6.0, ((0, 128),))
    key_projection = bell_draw(keys[1], (MODEL_WIDTH, KVW), MODEL_WIDTH ** -0.5, 0.09375)
    value_projection = bell_draw(keys[2], (MODEL_WIDTH, KVW), MODEL_WIDTH ** -0.5, 0.09375)
    key_norm_gain = jnp.clip(1.0 + 0.18 * jax.random.normal(keys[3], (HEAD_WIDTH,), jnp.float32), 0.1, 1.9)
    hidden = bell_draw(own_keys[4], (REQUEST_TOTAL, MODEL_WIDTH), 1.0, 6.0, ((0, 64), (1, 2)))
    shared_query_base = draw_shared_query_base(jax.random.fold_in(jax.random.fold_in(keys[10], part), 71), part)
    adapter_down_matrix = bell_draw(keys[6], (ADAPTER_TOTAL, MODEL_WIDTH, ADAPTER_RANK), MODEL_WIDTH ** -0.5, 0.09375, ((0, 64),))
    adapter_up_matrix = bell_draw(keys[7], (ADAPTER_TOTAL, ADAPTER_RANK, QUERY_WIDTH), ADAPTER_RANK ** -0.5, 1.5, ((0, 64),))
    tenant_adapter_index_keys = jax.random.split(jax.random.fold_in(own_keys[8], 1), REQUEST_TOTAL // REQ_DEV)
    tenant_adapter_index_turns = jax.random.permutation(jax.random.fold_in(own_keys[8], 3), REQUEST_TOTAL // REQ_DEV)
    tenant_adapter_index = jax.vmap(lambda own, number: assign_block(jax.random.fold_in(own_keys[8], 2), own, number, REQ_DEV, ADAPTER_TOTAL, 1, MOST, 2))(tenant_adapter_index_keys, tenant_adapter_index_turns).reshape((REQUEST_TOTAL, 1))
    used_tile_count = place_ends(jax.random.randint(own_keys[9], (REQUEST_TOTAL,), 1, TILE_SLOTS + 1), jax.random.fold_in(own_keys[9], 1), 1, TILE_SLOTS).astype(jnp.int32)
    return dict(images=images, key_projection=key_projection, value_projection=value_projection, key_norm_gain=key_norm_gain, hidden=hidden, shared_query_base=shared_query_base, adapter_down_matrix=adapter_down_matrix, adapter_up_matrix=adapter_up_matrix, tenant_adapter_index=tenant_adapter_index, used_tile_count=used_tile_count)


def reference(images, key_projection, value_projection, key_norm_gain, hidden, shared_query_base, adapter_down_matrix, adapter_up_matrix, tenant_adapter_index, used_tile_count):
    flattened_rows = images.reshape(REQUEST_TOTAL * TILE_SLOTS * TILE_TOKENS, MODEL_WIDTH)
    unnormed_keys = jnp.dot(flattened_rows, key_projection, preferred_element_type=jnp.float32).reshape(REQUEST_TOTAL, TILE_SLOTS * TILE_TOKENS, KEY_VALUE_HEADS, HEAD_WIDTH)
    key_scale = lax.rsqrt(lax.optimization_barrier(jnp.mean(unnormed_keys * unnormed_keys, axis=-1, keepdims=True)) + 1e-06)
    keys_all = (unnormed_keys * key_scale * key_norm_gain.astype(jnp.float32)).astype(jnp.bfloat16)
    gathered_values = jnp.dot(flattened_rows, value_projection, preferred_element_type=jnp.float32).astype(jnp.bfloat16)
    gathered_values = gathered_values.reshape(REQUEST_TOTAL, TILE_SLOTS * TILE_TOKENS, KEY_VALUE_HEADS, HEAD_WIDTH)
    owner_hot = (tenant_adapter_index[:, 0:1] == jnp.arange(ADAPTER_TOTAL, dtype=jnp.int32)[None, :]).astype(jnp.float32)
    widened_down_matrix = jnp.transpose(adapter_down_matrix, (1, 0, 2)).reshape(MODEL_WIDTH, ADAPTER_TOTAL * ADAPTER_RANK)
    low_all = jnp.dot(hidden, widened_down_matrix, preferred_element_type=jnp.float32).reshape(REQUEST_TOTAL, ADAPTER_TOTAL, ADAPTER_RANK)
    reduced_rank_part = lax.optimization_barrier(jnp.sum(low_all * owner_hot[:, :, None], axis=1))
    widened_reduced_part = owner_hot.astype(jnp.bfloat16)[:, :, None] * reduced_rank_part.astype(jnp.bfloat16)[:, None, :]
    adapter_query_delta = jnp.dot(widened_reduced_part.reshape(REQUEST_TOTAL, ADAPTER_TOTAL * ADAPTER_RANK), adapter_up_matrix.reshape(ADAPTER_TOTAL * ADAPTER_RANK, QUERY_WIDTH), preferred_element_type=jnp.float32).astype(jnp.bfloat16)
    query_rows = (shared_query_base.astype(jnp.float32) + adapter_query_delta.astype(jnp.float32)).astype(jnp.bfloat16)
    query_group_width = QUERY_HEADS // KEY_VALUE_HEADS
    query_four_axes = query_rows.reshape(REQUEST_TOTAL, KEY_VALUE_HEADS, query_group_width, HEAD_WIDTH).astype(jnp.float32)
    scores = jnp.einsum('rkgd,rjkd->rkgj', query_four_axes, keys_all.astype(jnp.float32)) / math.sqrt(HEAD_WIDTH)
    position = jnp.arange(TILE_SLOTS * TILE_TOKENS, dtype=jnp.int32) // TILE_TOKENS
    valid_rows = position[None, :] < used_tile_count[:, None]
    key_mask = valid_rows[:, None, None, :]
    scores = jnp.where(key_mask, scores, -jnp.inf)
    score_peak = lax.optimization_barrier(jnp.max(scores, axis=-1, keepdims=True))
    weights = jnp.exp(scores - score_peak)
    weight_total = lax.optimization_barrier(jnp.sum(weights, axis=-1))
    rounded = lax.optimization_barrier(weights.astype(jnp.bfloat16)).astype(jnp.float32)
    weighted = jnp.einsum('rkgj,rjkd->rkgd', rounded, gathered_values.astype(jnp.float32))
    attended = (weighted / weight_total[..., None]).reshape(REQUEST_TOTAL, QUERY_WIDTH).astype(jnp.bfloat16)
    return attended
```

```python
import functools
import math

import jax
import jax.numpy as jnp
from jax import lax
from jax.experimental import pallas as pl
from jax.experimental.pallas import tpu as pltpu
from jax.sharding import PartitionSpec as P

TILE_TOKENS = 3
CHUNK = 16
SLOTS = 4


def project_kernel(heads, size, x_ref, wk_ref, wv_ref, gain_ref, keys_ref, values_ref):
    x = x_ref[...]
    raw = jnp.dot(x, wk_ref[...], preferred_element_type=jnp.float32)
    for h in range(heads):
        part = raw[:, h * size : (h + 1) * size]
        scale = lax.rsqrt(jnp.mean(part * part, axis=-1, keepdims=True) + 1e-06)
        keys_ref[:, h * size : (h + 1) * size] = (part * scale * gain_ref[...]).astype(jnp.bfloat16)
    values_ref[...] = jnp.dot(x, wv_ref[...], preferred_element_type=jnp.float32).astype(jnp.bfloat16)


def project(x, wk, wv, gain):
    rows, width = x.shape
    kvw = wk.shape[1]
    size = gain.shape[1]
    tile = rows // 6 if rows % 6 == 0 and (rows // 6) % 16 == 0 else rows
    whole = lambda i: (0, 0)
    return pl.pallas_call(
        functools.partial(project_kernel, kvw // size, size),
        grid=(rows // tile,),
        in_specs=[
            pl.BlockSpec((tile, width), lambda i: (i, 0)),
            pl.BlockSpec((width, kvw), whole),
            pl.BlockSpec((width, kvw), whole),
            pl.BlockSpec((1, size), whole),
        ],
        out_specs=[pl.BlockSpec((tile, kvw), lambda i: (i, 0))] * 2,
        out_shape=[jax.ShapeDtypeStruct((rows, kvw), jnp.bfloat16)] * 2,
        cost_estimate=pl.CostEstimate(
            flops=4 * rows * width * kvw,
            bytes_accessed=2 * (rows * width + 2 * width * kvw + 2 * rows * kvw),
            transcendentals=0,
        ),
        name="project",
    )(x, wk, wv, gain)


def attend_kernel(requests, tokens, heads, group, size, q_ref, k_ref, v_ref, valid_ref, out_ref):
    wide = tokens * CHUNK
    row = lax.broadcasted_iota(jnp.int32, (group * CHUNK, wide), 0)
    col = lax.broadcasted_iota(jnp.int32, (group * CHUNK, wide), 1)
    same = (row % CHUNK) == (col % CHUNK)
    for c in range(requests // CHUNK):
        rows = slice(c * CHUNK, (c + 1) * CHUNK)
        use = same & (valid_ref[c : c + 1, :] > 0.0)
        for h in range(heads):
            lanes = slice(h * size, (h + 1) * size)
            q = jnp.concatenate(
                [
                    q_ref[rows, (h * group + g) * size : (h * group + g + 1) * size]
                    for g in range(group)
                ],
                axis=0,
            )
            k = k_ref[:, rows, lanes].reshape(wide, size)
            v = v_ref[:, rows, lanes].reshape(wide, size)
            scores = lax.dot_general(
                q, k, (((1,), (1,)), ((), ())), preferred_element_type=jnp.float32
            ) / math.sqrt(size)
            scores = jnp.where(use, scores, -jnp.inf)
            weights = jnp.exp(scores - jnp.max(scores, axis=-1, keepdims=True))
            total = jnp.sum(weights, axis=-1, keepdims=True)
            weighted = jnp.dot(weights.astype(jnp.bfloat16), v, preferred_element_type=jnp.float32)
            done = (weighted / total).astype(jnp.bfloat16)
            for g in range(group):
                out_ref[rows, (h * group + g) * size : (h * group + g + 1) * size] = done[
                    g * CHUNK : (g + 1) * CHUNK
                ]


def attend(q, keys, values, valid, size):
    tokens, requests, kvw = keys.shape
    heads = kvw // size
    group = q.shape[1] // kvw
    return pl.pallas_call(
        functools.partial(attend_kernel, requests, tokens, heads, group, size),
        out_shape=jax.ShapeDtypeStruct(q.shape, jnp.bfloat16),
        in_specs=[pl.BlockSpec(memory_space=pltpu.VMEM)] * 4,
        out_specs=pl.BlockSpec(memory_space=pltpu.VMEM),
        cost_estimate=pl.CostEstimate(
            flops=4 * q.size * tokens * CHUNK,
            bytes_accessed=4 * q.size + 4 * keys.size,
            transcendentals=0,
        ),
        name="attend",
    )(q, keys, values, valid)


def on_device(
    images,
    key_projection,
    value_projection,
    key_norm_gain,
    hidden,
    shared_query_base,
    adapter_down_matrix,
    adapter_up_matrix,
    tenant_adapter_index,
    used_tile_count,
):
    requests, half_model = hidden.shape
    half_query = shared_query_base.shape[1]
    size = key_norm_gain.shape[0]
    banks = lax.axis_size("aa")
    swap = [(0, 1), (1, 0)]
    ours = lax.axis_index("ba")

    owner = tenant_adapter_index[:, 0]
    hot = owner[:, None] == jnp.arange(banks, dtype=jnp.int32)[None, :]
    lower = jnp.arange(requests)[:, None] > jnp.arange(requests)[None, :]
    before = jnp.dot(
        lower.astype(jnp.bfloat16), hot.astype(jnp.bfloat16), preferred_element_type=jnp.float32
    )
    place = jnp.sum(jnp.where(hot, before, 0.0), axis=1).astype(jnp.int32)
    slots = banks * SLOTS
    slot = owner * SLOTS + place
    placing = (slot[:, None] == jnp.arange(slots, dtype=jnp.int32)[None, :]).astype(jnp.bfloat16)

    packed = lax.dot_general(
        placing, hidden, (((0,), (0,)), ((), ())), preferred_element_type=jnp.float32
    ).astype(jnp.bfloat16)
    rows_in = lax.all_to_all(
        packed.reshape(banks, SLOTS, half_model), "aa", 0, 0, tiled=True
    ).reshape(slots, half_model)

    down = lax.dynamic_slice_in_dim(
        adapter_down_matrix[0].T, ours * half_model, half_model, 1
    )
    up = lax.dynamic_slice_in_dim(adapter_up_matrix[0], ours * half_query, half_query, 1)

    here, tokens, width = images.shape
    x = images.transpose(1, 0, 2).reshape(tokens * here, width)
    keys, values = project(x, key_projection, value_projection, key_norm_gain[None, :])

    low = lax.dot_general(
        rows_in, down, (((1,), (1,)), ((), ())), preferred_element_type=jnp.float32
    )
    low = low + lax.ppermute(low, "ba", swap)
    raised = jnp.dot(low.astype(jnp.bfloat16), up, preferred_element_type=jnp.float32).astype(
        jnp.bfloat16
    )
    back = lax.all_to_all(
        raised.reshape(banks, SLOTS, half_query), "aa", 0, 0, tiled=True
    ).reshape(slots, half_query)
    delta = jnp.dot(placing, back, preferred_element_type=jnp.float32)
    query = (shared_query_base.astype(jnp.float32) + delta).astype(jnp.bfloat16)
    kept = lax.dynamic_slice_in_dim(query, ours * here, here, 0)
    sent = lax.dynamic_slice_in_dim(query, (1 - ours) * here, here, 0)
    got = lax.ppermute(sent, "ba", swap)
    first = jnp.where(ours == 0, kept, got)
    second = jnp.where(ours == 0, got, kept)
    q = jnp.concatenate([first, second], axis=1)

    position = jnp.arange(tokens, dtype=jnp.int32) // TILE_TOKENS
    valid = position[None, :, None] < used_tile_count.reshape(here // CHUNK, 1, CHUNK)
    valid = valid.astype(jnp.float32).reshape(here // CHUNK, tokens * CHUNK)
    return attend(
        q,
        keys.reshape(tokens, here, -1),
        values.reshape(tokens, here, -1),
        valid,
        size,
    )


def solution(mesh):
    placed = (
        P(("ga", "aa", "ba"), None, None),
        P(),
        P(),
        P(),
        P(("ga", "aa"), "ba"),
        P(("ga", "aa"), "ba"),
        P("aa", None, None),
        P("aa", None, None),
        P(("ga", "aa"), None),
        P(("ga", "aa", "ba")),
    )
    return jax.shard_map(
        on_device,
        mesh=mesh,
        in_specs=placed,
        out_specs=P(("ga", "aa", "ba"), None),
        check_vma=False,
    )
```

```python
import functools
import math

import jax
import jax.numpy as jnp
from jax import lax
from jax.experimental import pallas as pl
from jax.experimental.pallas import tpu as pltpu
from jax.sharding import PartitionSpec as P

TILE_TOKENS = 3
CHUNK = 16
SLOTS = 4
VMEM = pl.BlockSpec(memory_space=pltpu.VMEM)
SMEM = pl.BlockSpec(memory_space=pltpu.SMEM)


def call(kernel, ins, out, name, flops, limit=24):
    outs = jax.tree.leaves(out)
    specs = [SMEM if v.ndim == 1 else VMEM for v in ins]
    return pl.pallas_call(
        kernel,
        out_shape=out,
        in_specs=specs,
        out_specs=jax.tree.map(lambda _: VMEM, out),
        compiler_params=pltpu.CompilerParams(vmem_limit_bytes=limit * 2**20),
        cost_estimate=pl.CostEstimate(
            flops=flops,
            bytes_accessed=sum(v.size * v.dtype.itemsize for v in [*ins, *outs]),
            transcendentals=0,
        ),
        name=name,
    )(*ins)


def project_kernel(heads, size, x_ref, wk_ref, wv_ref, gain_ref, keys_ref, values_ref):
    x = x_ref[...]
    raw = jnp.dot(x, wk_ref[...], preferred_element_type=jnp.float32)
    for h in range(heads):
        part = raw[:, h * size : (h + 1) * size]
        scale = lax.rsqrt(jnp.mean(part * part, axis=-1, keepdims=True) + 1e-06)
        keys_ref[:, h * size : (h + 1) * size] = (part * scale * gain_ref[...]).astype(jnp.bfloat16)
    values_ref[...] = jnp.dot(x, wv_ref[...], preferred_element_type=jnp.float32).astype(jnp.bfloat16)


def project(x, wk, wv, gain):
    rows, width = x.shape
    kvw = wk.shape[1]
    size = gain.shape[1]
    tile = rows // 6 if rows % 96 == 0 else rows
    whole = lambda i: (0, 0)
    return pl.pallas_call(
        functools.partial(project_kernel, kvw // size, size),
        grid=(rows // tile,),
        in_specs=[
            pl.BlockSpec((tile, width), lambda i: (i, 0)),
            pl.BlockSpec((width, kvw), whole),
            pl.BlockSpec((width, kvw), whole),
            pl.BlockSpec((1, size), whole),
        ],
        out_specs=[pl.BlockSpec((tile, kvw), lambda i: (i, 0))] * 2,
        out_shape=[jax.ShapeDtypeStruct((rows, kvw), jnp.bfloat16)] * 2,
        compiler_params=pltpu.CompilerParams(vmem_limit_bytes=40 * 2**20),
        cost_estimate=pl.CostEstimate(
            flops=4 * rows * width * kvw,
            bytes_accessed=2 * (rows * width + 2 * width * kvw + 2 * rows * kvw),
            transcendentals=0,
        ),
        name="project",
    )(x, wk, wv, gain)


def pack_kernel(side, core_ref, owner_ref, mine_ref, other_ref, bank_ref, out_ref, slot_ref):
    requests = owner_ref.shape[1]
    held = side // 2 * SLOTS
    core = core_ref[0]
    names = owner_ref[...]
    across = jnp.broadcast_to(names.astype(jnp.float32), (requests, requests))
    down = jnp.transpose(across)
    low = lax.broadcasted_iota(jnp.int32, (requests, requests), 0)
    high = lax.broadcasted_iota(jnp.int32, (requests, requests), 1)
    earlier = jnp.where((across == down) & (low < high), 1.0, 0.0)
    rank = jnp.sum(earlier, axis=0, keepdims=True).astype(jnp.int32)
    column = names % side
    line = names // side
    peer = jnp.where(core == 0, column, line)
    which = jnp.where(core == 0, line, column) // 2
    slot = jnp.where((column + line) % 2 == core, peer * held + which * SLOTS + rank, -1)
    slot_ref[...] = jnp.broadcast_to(slot, slot_ref.shape)
    row = lax.broadcasted_iota(jnp.int32, (side * held, requests), 0)
    placing = jnp.where(row == slot, 1.0, 0.0).astype(jnp.bfloat16)
    mine = jnp.dot(placing, mine_ref[...], preferred_element_type=jnp.float32).astype(jnp.bfloat16)
    other = jnp.dot(placing, other_ref[...], preferred_element_type=jnp.float32).astype(
        jnp.bfloat16
    )
    for p in range(side):
        out_ref[p, :held] = mine[p * held : (p + 1) * held]
        out_ref[p, held : 2 * held] = other[p * held : (p + 1) * held]
        out_ref[p, 2 * held :] = bank_ref[...]


def raise_kernel(side, rank, rows_ref, bank_ref, out_ref):
    held = side // 2 * SLOTS
    half = rank // 2
    width = rows_ref.shape[2]
    mine = rows_ref[:, :held].reshape(side * held, width)
    other = rows_ref[:, held : 2 * held].reshape(side * held, width)
    first = bank_ref[:, :half].reshape(side * half, width)
    second = bank_ref[:, half : 2 * half].reshape(side * half, width)
    up = bank_ref[:, 2 * half :].reshape(side * half, width)
    contract = (((1,), (1,)), ((), ()))
    low = lax.dot_general(mine, first, contract, preferred_element_type=jnp.float32)
    low = low + lax.dot_general(other, second, contract, preferred_element_type=jnp.float32)
    row = lax.broadcasted_iota(jnp.int32, low.shape, 0)
    col = lax.broadcasted_iota(jnp.int32, low.shape, 1)
    low = jnp.where((row // SLOTS) % (side // 2) == col // rank, low, 0.0).astype(jnp.bfloat16)
    raised = jnp.dot(low, up, preferred_element_type=jnp.float32).astype(jnp.bfloat16)
    out_ref[...] = raised.reshape(side, held, width)


def unpack_kernel(core_ref, slot_ref, back_ref, mine_ref, other_ref, whole):
    requests = slot_ref.shape[1]
    here = mine_ref.shape[0]
    core = core_ref[0]
    slots = back_ref.shape[0]
    row = lax.broadcasted_iota(jnp.int32, (slots, requests), 0)
    placing = jnp.where(row == slot_ref[:1], 1.0, 0.0).astype(jnp.bfloat16)
    whole[...] = lax.dot_general(
        placing, back_ref[...], (((0,), (0,)), ((), ())), preferred_element_type=jnp.float32
    )
    mine_ref[...] = whole[pl.ds(pl.multiple_of(core * here, here), here)].astype(jnp.bfloat16)
    other_ref[...] = whole[pl.ds(pl.multiple_of((1 - core) * here, here), here)].astype(
        jnp.bfloat16
    )


def attend_kernel(
    tokens, heads, group, size, mine_ref, got_ref, base_ref, k_ref, v_ref, valid_ref, out_ref
):
    requests = base_ref.shape[0]
    wide = tokens * CHUNK
    row = lax.broadcasted_iota(jnp.int32, (group * CHUNK, wide), 0)
    col = lax.broadcasted_iota(jnp.int32, (group * CHUNK, wide), 1)
    same = (row % CHUNK) == (col % CHUNK)
    delta = mine_ref[...].astype(jnp.float32) + got_ref[...].astype(jnp.float32)
    query = (base_ref[...].astype(jnp.float32) + delta).astype(jnp.bfloat16)
    for c in range(requests // CHUNK):
        rows = slice(c * CHUNK, (c + 1) * CHUNK)
        use = same & (valid_ref[c : c + 1, :] > 0.0)
        scores = []
        for h in range(heads):
            q = jnp.concatenate(
                [
                    query[rows, (h * group + g) * size : (h * group + g + 1) * size]
                    for g in range(group)
                ],
                axis=0,
            )
            k = k_ref[:, rows, h * size : (h + 1) * size].reshape(wide, size)
            scores.append(
                lax.dot_general(q, k, (((1,), (1,)), ((), ())), preferred_element_type=jnp.float32)
                / math.sqrt(size)
            )
        done = []
        for h in range(heads):
            masked = jnp.where(use, scores[h], -jnp.inf)
            weights = jnp.exp(masked - jnp.max(masked, axis=-1, keepdims=True))
            total = jnp.sum(weights, axis=-1, keepdims=True)
            v = v_ref[:, rows, h * size : (h + 1) * size].reshape(wide, size)
            weighted = jnp.dot(weights.astype(jnp.bfloat16), v, preferred_element_type=jnp.float32)
            done.append((weighted / total).astype(jnp.bfloat16))
        for h in range(heads):
            for g in range(group):
                out_ref[rows, (h * group + g) * size : (h * group + g + 1) * size] = done[h][
                    g * CHUNK : (g + 1) * CHUNK
                ]


def on_device(
    images,
    key_projection,
    value_projection,
    key_norm_gain,
    hidden,
    shared_query_base,
    adapter_down_matrix,
    adapter_up_matrix,
    tenant_adapter_index,
    used_tile_count,
):
    requests, half_model = hidden.shape
    half_query = shared_query_base.shape[1]
    size = key_norm_gain.shape[0]
    rank, width_query = adapter_up_matrix.shape[1:]
    here, tokens, width = images.shape
    banks = lax.axis_size("aa")
    side = math.isqrt(banks)
    assert side * side == banks and width_query == half_model
    held = side // 2 * SLOTS
    half = rank // 2
    both = ("aa", "ba")
    spot = range(side)
    lines = [[2 * (y * side + x) for x in spot] for y in spot]
    lines += [[2 * (y * side + x) + 1 for y in spot] for x in spot]
    beside = [(line[i], line[i ^ 1]) for line in lines for i in spot]
    swap = [(0, 1), (1, 0)]
    core = lax.axis_index("ba")
    bank = lax.axis_index("aa")
    column, line = bank % side, bank // side
    position = jnp.where(core == 0, column, line)
    flag = core.astype(jnp.int32).reshape(1)

    far_hidden = lax.ppermute(hidden, "ba", swap)

    halves = adapter_down_matrix[0].T.reshape(2, half, 2, half_model)
    whole = jnp.concatenate(
        [
            jnp.where(core == 0, halves[:, :, 1], halves[:, :, 0]),
            jnp.where(core == 0, halves[:, :, 0], halves[:, :, 1]),
            adapter_up_matrix[0].reshape(2, half, width_query),
        ],
        axis=1,
    )
    odd = position % 2 == 1
    ours = jnp.where(odd, whole[1], whole[0])
    theirs = lax.ppermute(jnp.where(odd, whole[0], whole[1]), both, beside)
    sent_bank = jnp.where((column + line) % 2 == 1 - core, ours, theirs)

    packed, slot = call(
        functools.partial(pack_kernel, side),
        [flag, tenant_adapter_index.reshape(1, requests), hidden, far_hidden, sent_bank],
        [
            jax.ShapeDtypeStruct((side, 2 * held + 3 * half, half_model), jnp.bfloat16),
            jax.ShapeDtypeStruct((8, requests), jnp.int32),
        ],
        "pack",
        4 * side * held * requests * half_model,
    )
    received = lax.all_to_all(packed, both, 0, 0, axis_index_groups=lines, tiled=True)

    x = images.transpose(1, 0, 2).reshape(tokens * here, width)
    keys, values = project(x, key_projection, value_projection, key_norm_gain[None, :])
    kept = lax.dynamic_slice_in_dim(shared_query_base, core * here, here, 0)
    sent = lax.dynamic_slice_in_dim(shared_query_base, (1 - core) * here, here, 0)
    got = lax.ppermute(sent, "ba", swap)
    base = jnp.concatenate(
        [jnp.where(core == 0, kept, got), jnp.where(core == 0, got, kept)], axis=1
    )
    tile = jnp.arange(tokens, dtype=jnp.int32) // TILE_TOKENS
    valid = tile[None, :, None] < used_tile_count.reshape(here // CHUNK, 1, CHUNK)
    valid = valid.astype(jnp.float32).reshape(here // CHUNK, tokens * CHUNK)
    received, keys, values, base, valid = lax.optimization_barrier(
        (received, keys, values, base, valid)
    )

    bank_rows = lax.ppermute(received[:, 2 * held :], "ba", swap)
    raised = call(
        functools.partial(raise_kernel, side, rank),
        [received, bank_rows],
        jax.ShapeDtypeStruct((side, held, width_query), jnp.bfloat16),
        "raise",
        6 * side * held * side * half * half_model,
    )
    back = lax.all_to_all(raised, both, 0, 0, axis_index_groups=lines, tiled=True)
    back = back.reshape(side * held, width_query)
    part = jax.ShapeDtypeStruct((here, width_query), jnp.bfloat16)
    mine, other = pl.pallas_call(
        unpack_kernel,
        out_shape=[part, part],
        in_specs=[SMEM, VMEM, VMEM],
        out_specs=[VMEM, VMEM],
        scratch_shapes=[pltpu.VMEM((requests, width_query), jnp.float32)],
        compiler_params=pltpu.CompilerParams(vmem_limit_bytes=24 * 2**20),
        cost_estimate=pl.CostEstimate(
            flops=2 * side * held * requests * width_query,
            bytes_accessed=4 * back.size,
            transcendentals=0,
        ),
        name="unpack",
    )(flag, slot, back)
    rest = lax.ppermute(other, "ba", swap)
    kvw = key_projection.shape[1]
    return call(
        functools.partial(attend_kernel, tokens, kvw // size, width_query // kvw, size),
        [
            mine,
            rest,
            base,
            keys.reshape(tokens, here, kvw),
            values.reshape(tokens, here, kvw),
            valid,
        ],
        jax.ShapeDtypeStruct((here, width_query), jnp.bfloat16),
        "attend",
        4 * here * width_query * tokens * CHUNK,
    )


def solution(mesh):
    placed = (
        P(("ga", "aa", "ba"), None, None),
        P(),
        P(),
        P(),
        P(("ga", "aa"), "ba"),
        P(("ga", "aa"), "ba"),
        P("aa", None, None),
        P("aa", None, None),
        P(("ga", "aa"), None),
        P(("ga", "aa", "ba")),
    )
    return jax.shard_map(
        on_device,
        mesh=mesh,
        in_specs=placed,
        out_specs=P(("ga", "aa", "ba"), None),
        check_vma=False,
    )
```

```python
import functools
import math

import jax
import jax.numpy as jnp
from jax import lax
from jax.experimental import pallas as pl
from jax.experimental.pallas import tpu as pltpu
from jax.sharding import PartitionSpec as P

TILE_TOKENS = 3
CHUNK = 16
SLOTS = 4
VMEM = pl.BlockSpec(memory_space=pltpu.VMEM)
SMEM = pl.BlockSpec(memory_space=pltpu.SMEM)


def call(kernel, ins, out, flops, limit=24):
    outs = jax.tree.leaves(out)
    specs = [SMEM if v.ndim == 1 else VMEM for v in ins]
    return pl.pallas_call(
        kernel,
        out_shape=out,
        in_specs=specs,
        out_specs=jax.tree.map(lambda _: VMEM, out),
        compiler_params=pltpu.CompilerParams(vmem_limit_bytes=limit * 2**20),
        cost_estimate=pl.CostEstimate(
            flops=flops,
            bytes_accessed=sum(v.size * v.dtype.itemsize for v in [*ins, *outs]),
            transcendentals=0,
        ),
    )(*ins)


def project_kernel(heads, size, x_ref, wk_ref, wv_ref, gain_ref, keys_ref, values_ref):
    x = x_ref[...]
    raw = jnp.dot(x, wk_ref[...], preferred_element_type=jnp.float32)
    for h in range(heads):
        part = raw[:, h * size : (h + 1) * size]
        scale = lax.rsqrt(jnp.mean(part * part, axis=-1, keepdims=True) + 1e-06)
        keys_ref[:, h * size : (h + 1) * size] = (part * scale * gain_ref[...]).astype(jnp.bfloat16)
    values_ref[...] = jnp.dot(x, wv_ref[...], preferred_element_type=jnp.float32).astype(jnp.bfloat16)


def project(x, wk, wv, gain):
    rows, width = x.shape
    kvw = wk.shape[1]
    size = gain.shape[1]
    tile = rows // 6 if rows % 96 == 0 else rows
    whole = lambda i: (0, 0)
    return pl.pallas_call(
        functools.partial(project_kernel, kvw // size, size),
        grid=(rows // tile,),
        in_specs=[
            pl.BlockSpec((tile, width), lambda i: (i, 0)),
            pl.BlockSpec((width, kvw), whole),
            pl.BlockSpec((width, kvw), whole),
            pl.BlockSpec((1, size), whole),
        ],
        out_specs=[pl.BlockSpec((tile, kvw), lambda i: (i, 0))] * 2,
        out_shape=[jax.ShapeDtypeStruct((rows, kvw), jnp.bfloat16)] * 2,
        compiler_params=pltpu.CompilerParams(vmem_limit_bytes=40 * 2**20),
        cost_estimate=pl.CostEstimate(
            flops=4 * rows * width * kvw,
            bytes_accessed=2 * (rows * width + 2 * width * kvw + 2 * rows * kvw),
            transcendentals=0,
        ),
        name="project",
    )(x, wk, wv, gain)


def cut_kernel(half, at_ref, down_ref, up_ref, ours_ref, theirs_ref):
    core, odd = at_ref[0], at_ref[1]
    width = ours_ref.shape[1]

    def cut(out, low):
        rows = slice(low * half, (low + 1) * half)

        @pl.when(core == 0)
        def _():
            out[:half] = down_ref[rows, width:]
            out[half : 2 * half] = down_ref[rows, :width]

        @pl.when(core != 0)
        def _():
            out[:half] = down_ref[rows, :width]
            out[half : 2 * half] = down_ref[rows, width:]

        out[2 * half :] = up_ref[rows]

    @pl.when(odd == 0)
    def _():
        cut(ours_ref, 0)
        cut(theirs_ref, 1)

    @pl.when(odd != 0)
    def _():
        cut(ours_ref, 1)
        cut(theirs_ref, 0)


def placing_of(slot, slots):
    row = lax.broadcasted_iota(jnp.int32, (slots, slot.shape[1]), 0)
    return jnp.where(row == slot, 1.0, 0.0).astype(jnp.bfloat16)


def near_kernel(side, at_ref, names_ref, mine_ref, near_ref, slot_ref):
    requests = names_ref.shape[1]
    held = side // 2 * SLOTS
    core = at_ref[0]
    names = names_ref[...]
    across = jnp.broadcast_to(names.astype(jnp.float32), (requests, requests))
    down = jnp.transpose(across)
    low = lax.broadcasted_iota(jnp.int32, (requests, requests), 0)
    high = lax.broadcasted_iota(jnp.int32, (requests, requests), 1)
    earlier = jnp.where((across == down) & (low < high), 1.0, 0.0)
    rank = jnp.sum(earlier, axis=0, keepdims=True).astype(jnp.int32)
    column = names % side
    line = names // side
    peer = jnp.where(core == 0, line, column)
    which = jnp.where(core == 0, column, line) // 2
    slot = jnp.where((column + line) % 2 == 1 - core, peer * held + which * SLOTS + rank, -1)
    slot_ref[...] = jnp.broadcast_to(slot, slot_ref.shape)
    placing = placing_of(slot, side * held)
    near_ref[...] = jnp.dot(placing, mine_ref[...], preferred_element_type=jnp.float32).astype(
        jnp.bfloat16
    )


def far_kernel(side, at_ref, slot_ref, near_ref, other_ref, ours_ref, theirs_ref, out_ref):
    held = side // 2 * SLOTS
    placing = placing_of(slot_ref[:1], side * held)
    other = jnp.dot(placing, other_ref[...], preferred_element_type=jnp.float32).astype(
        jnp.bfloat16
    )
    bank = jnp.where(at_ref[2] == at_ref[0], ours_ref[...], theirs_ref[...])
    for p in range(side):
        out_ref[p, :held] = near_ref[p * held : (p + 1) * held]
        out_ref[p, held : 2 * held] = other[p * held : (p + 1) * held]
        out_ref[p, 2 * held :] = bank


def raise_kernel(side, rank, rows_ref, bank_ref, out_ref):
    held = side // 2 * SLOTS
    half = rank // 2
    width = rows_ref.shape[2]
    mine = rows_ref[:, :held].reshape(side * held, width)
    other = rows_ref[:, held : 2 * held].reshape(side * held, width)
    first = bank_ref[:, :half].reshape(side * half, width)
    second = bank_ref[:, half : 2 * half].reshape(side * half, width)
    up = bank_ref[:, 2 * half :].reshape(side * half, width)
    contract = (((1,), (1,)), ((), ()))
    low = lax.dot_general(mine, first, contract, preferred_element_type=jnp.float32)
    low = low + lax.dot_general(other, second, contract, preferred_element_type=jnp.float32)
    row = lax.broadcasted_iota(jnp.int32, low.shape, 0)
    col = lax.broadcasted_iota(jnp.int32, low.shape, 1)
    low = jnp.where((row // SLOTS) % (side // 2) == col // rank, low, 0.0).astype(jnp.bfloat16)
    raised = jnp.dot(low, up, preferred_element_type=jnp.float32).astype(jnp.bfloat16)
    out_ref[...] = raised.reshape(side, held, width)


def unpack_kernel(core_ref, slot_ref, back_ref, mine_ref, other_ref, whole):
    requests = slot_ref.shape[1]
    here = mine_ref.shape[0]
    core = core_ref[0]
    slots = back_ref.shape[0]
    row = lax.broadcasted_iota(jnp.int32, (slots, requests), 0)
    placing = jnp.where(row == slot_ref[:1], 1.0, 0.0).astype(jnp.bfloat16)
    whole[...] = lax.dot_general(
        placing, back_ref[...], (((0,), (0,)), ((), ())), preferred_element_type=jnp.float32
    )
    mine_ref[...] = whole[pl.ds(pl.multiple_of(core * here, here), here)].astype(jnp.bfloat16)
    other_ref[...] = whole[pl.ds(pl.multiple_of((1 - core) * here, here), here)].astype(
        jnp.bfloat16
    )


def attend_kernel(
    tokens, heads, group, size, mine_ref, got_ref, base_ref, k_ref, v_ref, valid_ref, out_ref
):
    requests = base_ref.shape[0]
    wide = tokens * CHUNK
    row = lax.broadcasted_iota(jnp.int32, (group * CHUNK, wide), 0)
    col = lax.broadcasted_iota(jnp.int32, (group * CHUNK, wide), 1)
    same = (row % CHUNK) == (col % CHUNK)
    delta = mine_ref[...].astype(jnp.float32) + got_ref[...].astype(jnp.float32)
    query = (base_ref[...].astype(jnp.float32) + delta).astype(jnp.bfloat16)
    for c in range(requests // CHUNK):
        rows = slice(c * CHUNK, (c + 1) * CHUNK)
        use = same & (valid_ref[c : c + 1, :] > 0.0)
        scores = []
        for h in range(heads):
            q = jnp.concatenate(
                [
                    query[rows, (h * group + g) * size : (h * group + g + 1) * size]
                    for g in range(group)
                ],
                axis=0,
            )
            k = k_ref[:, rows, h * size : (h + 1) * size].reshape(wide, size)
            scores.append(
                lax.dot_general(q, k, (((1,), (1,)), ((), ())), preferred_element_type=jnp.float32)
                / math.sqrt(size)
            )
        done = []
        for h in range(heads):
            masked = jnp.where(use, scores[h], -jnp.inf)
            weights = jnp.exp(masked - jnp.max(masked, axis=-1, keepdims=True))
            total = jnp.sum(weights, axis=-1, keepdims=True)
            v = v_ref[:, rows, h * size : (h + 1) * size].reshape(wide, size)
            weighted = jnp.dot(weights.astype(jnp.bfloat16), v, preferred_element_type=jnp.float32)
            done.append((weighted / total).astype(jnp.bfloat16))
        for h in range(heads):
            for g in range(group):
                out_ref[rows, (h * group + g) * size : (h * group + g + 1) * size] = done[h][
                    g * CHUNK : (g + 1) * CHUNK
                ]


def on_device(
    images,
    key_projection,
    value_projection,
    key_norm_gain,
    hidden,
    shared_query_base,
    adapter_down_matrix,
    adapter_up_matrix,
    tenant_adapter_index,
    used_tile_count,
):
    requests, half_model = hidden.shape
    size = key_norm_gain.shape[0]
    rank, width_query = adapter_up_matrix.shape[1:]
    here, tokens, width = images.shape
    banks = lax.axis_size("aa")
    side = math.isqrt(banks)
    assert side * side == banks and width_query == half_model
    held = side // 2 * SLOTS
    half = rank // 2
    both = ("aa", "ba")
    spot = range(side)
    lines = [[2 * (y * side + x) for y in spot] for x in spot]
    lines += [[2 * (y * side + x) + 1 for x in spot] for y in spot]
    beside = [
        (line[i], line[i ^ 1])
        for line in lines
        for i in spot
        if (line[i] // 2 // side + line[i] // 2 % side) % 2 == line[i] % 2
    ]
    swap = [(0, 1), (1, 0)]
    core = lax.axis_index("ba")
    bank = lax.axis_index("aa")
    column, line = bank % side, bank // side
    position = jnp.where(core == 0, line, column)
    flag = core.astype(jnp.int32).reshape(1)
    at = jnp.stack([core, position % 2, (column + line) % 2]).astype(jnp.int32)

    piece = jax.ShapeDtypeStruct((3 * half, half_model), jnp.bfloat16)
    ours, theirs = call(
        functools.partial(cut_kernel, half),
        [at, adapter_down_matrix[0].T, adapter_up_matrix[0]],
        [piece, piece],
        0,
    )
    theirs = lax.ppermute(theirs, both, beside)
    far_hidden = lax.ppermute(hidden, "ba", swap)
    near, slot = call(
        functools.partial(near_kernel, side),
        [at, tenant_adapter_index.reshape(1, requests), hidden],
        [
            jax.ShapeDtypeStruct((side * held, half_model), jnp.bfloat16),
            jax.ShapeDtypeStruct((8, requests), jnp.int32),
        ],
        2 * side * held * requests * half_model,
    )
    packed = call(
        functools.partial(far_kernel, side),
        [at, slot, near, far_hidden, ours, theirs],
        jax.ShapeDtypeStruct((side, 2 * held + 3 * half, half_model), jnp.bfloat16),
        2 * side * held * requests * half_model,
    )
    received = lax.all_to_all(packed, both, 0, 0, axis_index_groups=lines, tiled=True)

    x = images.transpose(1, 0, 2).reshape(tokens * here, width)
    keys, values = project(x, key_projection, value_projection, key_norm_gain[None, :])
    kept = lax.dynamic_slice_in_dim(shared_query_base, core * here, here, 0)
    sent = lax.dynamic_slice_in_dim(shared_query_base, (1 - core) * here, here, 0)
    got = lax.ppermute(sent, "ba", swap)
    base = jnp.concatenate(
        [jnp.where(core == 0, kept, got), jnp.where(core == 0, got, kept)], axis=1
    )
    tile = jnp.arange(tokens, dtype=jnp.int32) // TILE_TOKENS
    valid = tile[None, :, None] < used_tile_count.reshape(here // CHUNK, 1, CHUNK)
    valid = valid.astype(jnp.float32).reshape(here // CHUNK, tokens * CHUNK)
    received, keys, values, base, valid = lax.optimization_barrier(
        (received, keys, values, base, valid)
    )

    bank_rows = lax.ppermute(received[:, 2 * held :], "ba", swap)
    raised = call(
        functools.partial(raise_kernel, side, rank),
        [received, bank_rows],
        jax.ShapeDtypeStruct((side, held, width_query), jnp.bfloat16),
        6 * side * held * side * half * half_model,
    )
    back = lax.all_to_all(raised, both, 0, 0, axis_index_groups=lines, tiled=True)
    back = back.reshape(side * held, width_query)
    part = jax.ShapeDtypeStruct((here, width_query), jnp.bfloat16)
    mine, other = pl.pallas_call(
        unpack_kernel,
        out_shape=[part, part],
        in_specs=[SMEM, VMEM, VMEM],
        out_specs=[VMEM, VMEM],
        scratch_shapes=[pltpu.VMEM((requests, width_query), jnp.float32)],
        compiler_params=pltpu.CompilerParams(vmem_limit_bytes=24 * 2**20),
        cost_estimate=pl.CostEstimate(
            flops=2 * side * held * requests * width_query,
            bytes_accessed=4 * back.size,
            transcendentals=0,
        ),
        name="unpack",
    )(flag, slot, back)
    rest = lax.ppermute(other, "ba", swap)
    kvw = key_projection.shape[1]
    return call(
        functools.partial(attend_kernel, tokens, kvw // size, width_query // kvw, size),
        [
            mine,
            rest,
            base,
            keys.reshape(tokens, here, kvw),
            values.reshape(tokens, here, kvw),
            valid,
        ],
        jax.ShapeDtypeStruct((here, width_query), jnp.bfloat16),
        4 * here * width_query * tokens * CHUNK,
    )


def solution(mesh):
    placed = (
        P(("ga", "aa", "ba"), None, None),
        P(),
        P(),
        P(),
        P(("ga", "aa"), "ba"),
        P(("ga", "aa"), "ba"),
        P("aa", None, None),
        P("aa", None, None),
        P(("ga", "aa"), None),
        P(("ga", "aa", "ba")),
    )
    return jax.shard_map(
        on_device,
        mesh=mesh,
        in_specs=placed,
        out_specs=P(("ga", "aa", "ba"), None),
        check_vma=False,
    )
```

```python
import functools
import math

import jax
import jax.numpy as jnp
from jax import lax
from jax.experimental import pallas as pl
from jax.experimental.pallas import tpu as pltpu
from jax.sharding import PartitionSpec as P

TILE_TOKENS = 3
CHUNK = 16
SLOTS = 4
VMEM = pl.BlockSpec(memory_space=pltpu.VMEM)
SMEM = pl.BlockSpec(memory_space=pltpu.SMEM)


def call(kernel, ins, out, flops, limit=24):
    outs = jax.tree.leaves(out)
    specs = [SMEM if v.ndim == 1 else VMEM for v in ins]
    return pl.pallas_call(
        kernel,
        out_shape=out,
        in_specs=specs,
        out_specs=jax.tree.map(lambda _: VMEM, out),
        compiler_params=pltpu.CompilerParams(vmem_limit_bytes=limit * 2**20),
        cost_estimate=pl.CostEstimate(
            flops=flops,
            bytes_accessed=sum(v.size * v.dtype.itemsize for v in [*ins, *outs]),
            transcendentals=0,
        ),
    )(*ins)


def project_kernel(heads, size, x_ref, wk_ref, wv_ref, gain_ref, keys_ref, values_ref):
    x = x_ref[...]
    raw = jnp.dot(x, wk_ref[...], preferred_element_type=jnp.float32)
    for h in range(heads):
        part = raw[:, h * size : (h + 1) * size]
        scale = lax.rsqrt(jnp.mean(part * part, axis=-1, keepdims=True) + 1e-06)
        keys_ref[:, h * size : (h + 1) * size] = (part * scale * gain_ref[...]).astype(jnp.bfloat16)
    values_ref[...] = jnp.dot(x, wv_ref[...], preferred_element_type=jnp.float32).astype(jnp.bfloat16)


def project(x, wk, wv, gain):
    rows, width = x.shape
    kvw = wk.shape[1]
    size = gain.shape[1]
    tile = rows // 6 if rows % 96 == 0 else rows
    whole = lambda i: (0, 0)
    return pl.pallas_call(
        functools.partial(project_kernel, kvw // size, size),
        grid=(rows // tile,),
        in_specs=[
            pl.BlockSpec((tile, width), lambda i: (i, 0)),
            pl.BlockSpec((width, kvw), whole),
            pl.BlockSpec((width, kvw), whole),
            pl.BlockSpec((1, size), whole),
        ],
        out_specs=[pl.BlockSpec((tile, kvw), lambda i: (i, 0))] * 2,
        out_shape=[jax.ShapeDtypeStruct((rows, kvw), jnp.bfloat16)] * 2,
        compiler_params=pltpu.CompilerParams(vmem_limit_bytes=40 * 2**20),
        cost_estimate=pl.CostEstimate(
            flops=4 * rows * width * kvw,
            bytes_accessed=2 * (rows * width + 2 * width * kvw + 2 * rows * kvw),
            transcendentals=0,
        ),
        name="project",
    )(x, wk, wv, gain)


def placing_of(slot, slots):
    row = lax.broadcasted_iota(jnp.int32, (slots, slot.shape[1]), 0)
    return jnp.where(row == slot, 1.0, 0.0).astype(jnp.bfloat16)


def slot_kernel(side, at_ref, names_ref, slot_ref):
    requests = names_ref.shape[1]
    held = side // 2 * SLOTS
    core = at_ref[0]
    names = names_ref[...]
    across = jnp.broadcast_to(names.astype(jnp.float32), (requests, requests))
    down = jnp.transpose(across)
    low = lax.broadcasted_iota(jnp.int32, (requests, requests), 0)
    high = lax.broadcasted_iota(jnp.int32, (requests, requests), 1)
    earlier = jnp.where((across == down) & (low < high), 1.0, 0.0)
    rank = jnp.sum(earlier, axis=0, keepdims=True).astype(jnp.int32)
    column = names % side
    line = names // side
    peer = jnp.where(core == 0, line, column)
    which = jnp.where(core == 0, column, line) // 2
    slot = jnp.where((column + line) % 2 == 1 - core, peer * held + which * SLOTS + rank, -1)
    slot_ref[...] = jnp.broadcast_to(slot, slot_ref.shape)


def pack_kernel(
    side, at_ref, slot_ref, mine_ref, other_ref, down_ref, up_ref, next_down_ref, next_up_ref, out_ref
):
    held = side // 2 * SLOTS
    core, odd, owned = at_ref[0], at_ref[1], at_ref[2]
    width = other_ref.shape[1]
    half = down_ref.shape[0] // 2

    def cut(down, up, low):
        rows = slice(low * half, (low + 1) * half)
        left, right = down[rows, :width], down[rows, width:]
        piece = jnp.concatenate(
            [jnp.where(core == 0, right, left), jnp.where(core == 0, left, right), up[rows]], axis=0
        )
        for p in range(side):
            out_ref[p, 2 * held :] = piece

    for own, (down, up) in ((1, (down_ref, up_ref)), (0, (next_down_ref, next_up_ref))):
        for low in (0, 1):

            @pl.when((owned == own) & (odd == low))
            def _():
                cut(down, up, low)

    placing = placing_of(slot_ref[:1], side * held)
    for n, source in enumerate((mine_ref, other_ref)):
        placed = jnp.dot(placing, source[...], preferred_element_type=jnp.float32).astype(
            jnp.bfloat16
        )
        for p in range(side):
            out_ref[p, n * held : (n + 1) * held] = placed[p * held : (p + 1) * held]


def raise_kernel(side, rank, rows_ref, bank_ref, out_ref):
    held = side // 2 * SLOTS
    half = rank // 2
    width = rows_ref.shape[2]
    mine = rows_ref[:, :held].reshape(side * held, width)
    other = rows_ref[:, held : 2 * held].reshape(side * held, width)
    first = bank_ref[:, :half].reshape(side * half, width)
    second = bank_ref[:, half : 2 * half].reshape(side * half, width)
    up = bank_ref[:, 2 * half :].reshape(side * half, width)
    contract = (((1,), (1,)), ((), ()))
    low = lax.dot_general(mine, first, contract, preferred_element_type=jnp.float32)
    low = low + lax.dot_general(other, second, contract, preferred_element_type=jnp.float32)
    row = lax.broadcasted_iota(jnp.int32, low.shape, 0)
    col = lax.broadcasted_iota(jnp.int32, low.shape, 1)
    low = jnp.where((row // SLOTS) % (side // 2) == col // rank, low, 0.0).astype(jnp.bfloat16)
    raised = jnp.dot(low, up, preferred_element_type=jnp.float32).astype(jnp.bfloat16)
    out_ref[...] = raised.reshape(side, held, width)


def unpack_kernel(core_ref, slot_ref, back_ref, mine_ref, other_ref, whole):
    requests = slot_ref.shape[1]
    here = mine_ref.shape[0]
    core = core_ref[0]
    slots = back_ref.shape[0]
    row = lax.broadcasted_iota(jnp.int32, (slots, requests), 0)
    placing = jnp.where(row == slot_ref[:1], 1.0, 0.0).astype(jnp.bfloat16)
    whole[...] = lax.dot_general(
        placing, back_ref[...], (((0,), (0,)), ((), ())), preferred_element_type=jnp.float32
    )
    mine_ref[...] = whole[pl.ds(pl.multiple_of(core * here, here), here)].astype(jnp.bfloat16)
    other_ref[...] = whole[pl.ds(pl.multiple_of((1 - core) * here, here), here)].astype(
        jnp.bfloat16
    )


def attend_kernel(
    tokens, heads, group, size, mine_ref, got_ref, base_ref, k_ref, v_ref, valid_ref, out_ref
):
    requests = base_ref.shape[0]
    wide = tokens * CHUNK
    row = lax.broadcasted_iota(jnp.int32, (group * CHUNK, wide), 0)
    col = lax.broadcasted_iota(jnp.int32, (group * CHUNK, wide), 1)
    same = (row % CHUNK) == (col % CHUNK)
    delta = mine_ref[...].astype(jnp.float32) + got_ref[...].astype(jnp.float32)
    query = (base_ref[...].astype(jnp.float32) + delta).astype(jnp.bfloat16)
    for c in range(requests // CHUNK):
        rows = slice(c * CHUNK, (c + 1) * CHUNK)
        use = same & (valid_ref[c : c + 1, :] > 0.0)
        scores = []
        for h in range(heads):
            q = jnp.concatenate(
                [
                    query[rows, (h * group + g) * size : (h * group + g + 1) * size]
                    for g in range(group)
                ],
                axis=0,
            )
            k = k_ref[:, rows, h * size : (h + 1) * size].reshape(wide, size)
            scores.append(
                lax.dot_general(q, k, (((1,), (1,)), ((), ())), preferred_element_type=jnp.float32)
                / math.sqrt(size)
            )
        done = []
        for h in range(heads):
            masked = jnp.where(use, scores[h], -jnp.inf)
            weights = jnp.exp(masked - jnp.max(masked, axis=-1, keepdims=True))
            total = jnp.sum(weights, axis=-1, keepdims=True)
            v = v_ref[:, rows, h * size : (h + 1) * size].reshape(wide, size)
            weighted = jnp.dot(weights.astype(jnp.bfloat16), v, preferred_element_type=jnp.float32)
            done.append((weighted / total).astype(jnp.bfloat16))
        for h in range(heads):
            for g in range(group):
                out_ref[rows, (h * group + g) * size : (h * group + g + 1) * size] = done[h][
                    g * CHUNK : (g + 1) * CHUNK
                ]


def on_device(
    images,
    key_projection,
    value_projection,
    key_norm_gain,
    hidden,
    shared_query_base,
    adapter_down_matrix,
    adapter_up_matrix,
    tenant_adapter_index,
    used_tile_count,
):
    requests, half_model = hidden.shape
    size = key_norm_gain.shape[0]
    rank, width_query = adapter_up_matrix.shape[1:]
    here, tokens, width = images.shape
    banks = lax.axis_size("aa")
    side = math.isqrt(banks)
    assert side * side == banks and width_query == half_model
    held = side // 2 * SLOTS
    half = rank // 2
    both = ("aa", "ba")
    spot = range(side)
    lines = [[2 * (y * side + x) for y in spot] for x in spot]
    lines += [[2 * (y * side + x) + 1 for x in spot] for y in spot]
    beside = [
        (line[i] | 1, line[i ^ 1])
        for line in lines
        for i in spot
        if (line[i] // 2 // side + line[i] // 2 % side) % 2 == line[i] % 2
    ]
    swap = [(0, 1), (1, 0)]
    core = lax.axis_index("ba")
    bank = lax.axis_index("aa")
    column, line = bank % side, bank // side
    position = jnp.where(core == 0, line, column)
    flag = core.astype(jnp.int32).reshape(1)
    owned = (column + line) % 2 == core
    at = jnp.stack([core, position % 2, owned]).astype(jnp.int32)

    down, up = adapter_down_matrix[0].T, adapter_up_matrix[0]
    next_down = lax.ppermute(down, both, beside)
    next_up = lax.ppermute(up, both, beside)
    far_hidden = lax.ppermute(hidden, "ba", swap)
    slot = call(
        functools.partial(slot_kernel, side),
        [at, tenant_adapter_index.reshape(1, requests)],
        jax.ShapeDtypeStruct((8, requests), jnp.int32),
        2 * 10**10,
    )
    packed = call(
        functools.partial(pack_kernel, side),
        [at, slot, hidden, far_hidden, down, up, next_down, next_up],
        jax.ShapeDtypeStruct((side, 2 * held + 3 * half, half_model), jnp.bfloat16),
        4 * side * held * requests * half_model,
    )
    received = lax.all_to_all(packed, both, 0, 0, axis_index_groups=lines, tiled=True)

    x = images.transpose(1, 0, 2).reshape(tokens * here, width)
    keys, values = project(x, key_projection, value_projection, key_norm_gain[None, :])
    kept = lax.dynamic_slice_in_dim(shared_query_base, core * here, here, 0)
    sent = lax.dynamic_slice_in_dim(shared_query_base, (1 - core) * here, here, 0)
    got = lax.ppermute(sent, "ba", swap)
    base = jnp.concatenate(
        [jnp.where(core == 0, kept, got), jnp.where(core == 0, got, kept)], axis=1
    )
    tile = jnp.arange(tokens, dtype=jnp.int32) // TILE_TOKENS
    valid = tile[None, :, None] < used_tile_count.reshape(here // CHUNK, 1, CHUNK)
    valid = valid.astype(jnp.float32).reshape(here // CHUNK, tokens * CHUNK)
    received, keys, values, base, valid = lax.optimization_barrier(
        (received, keys, values, base, valid)
    )

    bank_rows = lax.ppermute(received[:, 2 * held :], "ba", swap)
    raised = call(
        functools.partial(raise_kernel, side, rank),
        [received, bank_rows],
        jax.ShapeDtypeStruct((side, held, width_query), jnp.bfloat16),
        6 * side * held * side * half * half_model,
    )
    back = lax.all_to_all(raised, both, 0, 0, axis_index_groups=lines, tiled=True)
    back = back.reshape(side * held, width_query)
    part = jax.ShapeDtypeStruct((here, width_query), jnp.bfloat16)
    mine, other = pl.pallas_call(
        unpack_kernel,
        out_shape=[part, part],
        in_specs=[SMEM, VMEM, VMEM],
        out_specs=[VMEM, VMEM],
        scratch_shapes=[pltpu.VMEM((requests, width_query), jnp.float32)],
        compiler_params=pltpu.CompilerParams(vmem_limit_bytes=24 * 2**20),
        cost_estimate=pl.CostEstimate(
            flops=2 * side * held * requests * width_query,
            bytes_accessed=4 * back.size,
            transcendentals=0,
        ),
        name="unpack",
    )(flag, slot, back)
    rest = lax.ppermute(other, "ba", swap)
    kvw = key_projection.shape[1]
    return call(
        functools.partial(attend_kernel, tokens, kvw // size, width_query // kvw, size),
        [
            mine,
            rest,
            base,
            keys.reshape(tokens, here, kvw),
            values.reshape(tokens, here, kvw),
            valid,
        ],
        jax.ShapeDtypeStruct((here, width_query), jnp.bfloat16),
        4 * here * width_query * tokens * CHUNK,
    )


def solution(mesh):
    placed = (
        P(("ga", "aa", "ba"), None, None),
        P(),
        P(),
        P(),
        P(("ga", "aa"), "ba"),
        P(("ga", "aa"), "ba"),
        P("aa", None, None),
        P("aa", None, None),
        P(("ga", "aa"), None),
        P(("ga", "aa", "ba")),
    )
    return jax.shard_map(
        on_device,
        mesh=mesh,
        in_specs=placed,
        out_specs=P(("ga", "aa", "ba"), None),
        check_vma=False,
    )
```

```python
import functools
import math

import jax
import jax.numpy as jnp
from jax import lax
from jax.experimental import pallas as pl
from jax.experimental.pallas import tpu as pltpu
from jax.sharding import PartitionSpec as P

TILE_TOKENS = 3
CHUNK = 16
SLOTS = 4
VMEM = pl.BlockSpec(memory_space=pltpu.VMEM)
SMEM = pl.BlockSpec(memory_space=pltpu.SMEM)


def call(kernel, ins, out, flops, limit=24):
    outs = jax.tree.leaves(out)
    specs = [SMEM if v.ndim == 1 else VMEM for v in ins]
    return pl.pallas_call(
        kernel,
        out_shape=out,
        in_specs=specs,
        out_specs=jax.tree.map(lambda _: VMEM, out),
        compiler_params=pltpu.CompilerParams(vmem_limit_bytes=limit * 2**20),
        cost_estimate=pl.CostEstimate(
            flops=flops,
            bytes_accessed=sum(v.size * v.dtype.itemsize for v in [*ins, *outs]),
            transcendentals=0,
        ),
    )(*ins)


def project_kernel(heads, size, x_ref, wk_ref, wv_ref, gain_ref, keys_ref, values_ref):
    x = x_ref[...]
    raw = jnp.dot(x, wk_ref[...], preferred_element_type=jnp.float32)
    for h in range(heads):
        part = raw[:, h * size : (h + 1) * size]
        scale = lax.rsqrt(jnp.mean(part * part, axis=-1, keepdims=True) + 1e-06)
        keys_ref[:, h * size : (h + 1) * size] = (part * scale * gain_ref[...]).astype(jnp.bfloat16)
    values_ref[...] = jnp.dot(x, wv_ref[...], preferred_element_type=jnp.float32).astype(jnp.bfloat16)


def project(x, wk, wv, gain):
    rows, width = x.shape
    kvw = wk.shape[1]
    size = gain.shape[1]
    tile = rows // 6 if rows % 96 == 0 else rows
    whole = lambda i: (0, 0)
    return pl.pallas_call(
        functools.partial(project_kernel, kvw // size, size),
        grid=(rows // tile,),
        in_specs=[
            pl.BlockSpec((tile, width), lambda i: (i, 0)),
            pl.BlockSpec((width, kvw), whole),
            pl.BlockSpec((width, kvw), whole),
            pl.BlockSpec((1, size), whole),
        ],
        out_specs=[pl.BlockSpec((tile, kvw), lambda i: (i, 0))] * 2,
        out_shape=[jax.ShapeDtypeStruct((rows, kvw), jnp.bfloat16)] * 2,
        compiler_params=pltpu.CompilerParams(vmem_limit_bytes=40 * 2**20),
        cost_estimate=pl.CostEstimate(
            flops=4 * rows * width * kvw,
            bytes_accessed=2 * (rows * width + 2 * width * kvw + 2 * rows * kvw),
            transcendentals=0,
        ),
        name="project",
    )(x, wk, wv, gain)


def placing_of(slot, slots):
    row = lax.broadcasted_iota(jnp.int32, (slots, slot.shape[1]), 0)
    return jnp.where(row == slot, 1.0, 0.0).astype(jnp.bfloat16)


def slot_kernel(side, at_ref, names_ref, slot_ref):
    requests = names_ref.shape[1]
    held = side // 2 * SLOTS
    core = at_ref[0]
    names = names_ref[...]
    across = jnp.broadcast_to(names.astype(jnp.float32), (requests, requests))
    down = jnp.transpose(across)
    low = lax.broadcasted_iota(jnp.int32, (requests, requests), 0)
    high = lax.broadcasted_iota(jnp.int32, (requests, requests), 1)
    earlier = jnp.where((across == down) & (low < high), 1.0, 0.0)
    rank = jnp.sum(earlier, axis=0, keepdims=True).astype(jnp.int32)
    column = names % side
    line = names // side
    peer = jnp.where(core == 0, line, column)
    which = jnp.where(core == 0, column, line) // 2
    slot = jnp.where((column + line) % 2 == 1 - core, peer * held + which * SLOTS + rank, -1)
    slot_ref[...] = jnp.broadcast_to(slot, slot_ref.shape)


def pack_kernel(
    side, at_ref, slot_ref, mine_ref, other_ref, down_ref, up_ref, next_down_ref, next_up_ref, out_ref
):
    held = side // 2 * SLOTS
    core, odd, owned = at_ref[0], at_ref[1], at_ref[2]
    width = other_ref.shape[1]
    half = down_ref.shape[0] // 2

    def cut(down, up, low):
        rows = slice(low * half, (low + 1) * half)
        left, right = down[rows, :width], down[rows, width:]
        piece = jnp.concatenate(
            [jnp.where(core == 0, right, left), jnp.where(core == 0, left, right), up[rows]], axis=0
        )
        for p in range(side):
            out_ref[p, 2 * held :] = piece

    for own, (down, up) in ((1, (down_ref, up_ref)), (0, (next_down_ref, next_up_ref))):
        for low in (0, 1):

            @pl.when((owned == own) & (odd == low))
            def _():
                cut(down, up, low)

    placing = placing_of(slot_ref[:1], side * held)
    for n, source in enumerate((mine_ref, other_ref)):
        placed = jnp.dot(placing, source[...], preferred_element_type=jnp.float32).astype(
            jnp.bfloat16
        )
        for p in range(side):
            out_ref[p, n * held : (n + 1) * held] = placed[p * held : (p + 1) * held]


def raise_kernel(side, rank, rows_ref, bank_ref, out_ref):
    held = side // 2 * SLOTS
    half = rank // 2
    width = rows_ref.shape[2]
    mine = rows_ref[:, :held].reshape(side * held, width)
    other = rows_ref[:, held : 2 * held].reshape(side * held, width)
    first = bank_ref[:, :half].reshape(side * half, width)
    second = bank_ref[:, half : 2 * half].reshape(side * half, width)
    up = bank_ref[:, 2 * half :].reshape(side * half, width)
    contract = (((1,), (1,)), ((), ()))
    low = lax.dot_general(mine, first, contract, preferred_element_type=jnp.float32)
    low = low + lax.dot_general(other, second, contract, preferred_element_type=jnp.float32)
    row = lax.broadcasted_iota(jnp.int32, low.shape, 0)
    col = lax.broadcasted_iota(jnp.int32, low.shape, 1)
    low = jnp.where((row // SLOTS) % (side // 2) == col // rank, low, 0.0).astype(jnp.bfloat16)
    raised = jnp.dot(low, up, preferred_element_type=jnp.float32).astype(jnp.bfloat16)
    out_ref[...] = raised.reshape(side, held, width)


def unpack_kernel(core_ref, slot_ref, back_ref, mine_ref, other_ref, whole):
    requests = slot_ref.shape[1]
    here = mine_ref.shape[0]
    core = core_ref[0]
    slots = back_ref.shape[0]
    row = lax.broadcasted_iota(jnp.int32, (slots, requests), 0)
    placing = jnp.where(row == slot_ref[:1], 1.0, 0.0).astype(jnp.bfloat16)
    whole[...] = lax.dot_general(
        placing, back_ref[...], (((0,), (0,)), ((), ())), preferred_element_type=jnp.float32
    )
    mine_ref[...] = whole[pl.ds(pl.multiple_of(core * here, here), here)].astype(jnp.bfloat16)
    other_ref[...] = whole[pl.ds(pl.multiple_of((1 - core) * here, here), here)].astype(
        jnp.bfloat16
    )


def attend_kernel(
    tokens, heads, group, size, mine_ref, got_ref, base_ref, k_ref, v_ref, valid_ref, out_ref
):
    requests = base_ref.shape[0]
    wide = tokens * CHUNK
    row = lax.broadcasted_iota(jnp.int32, (group * CHUNK, wide), 0)
    col = lax.broadcasted_iota(jnp.int32, (group * CHUNK, wide), 1)
    same = (row % CHUNK) == (col % CHUNK)
    delta = mine_ref[...].astype(jnp.float32) + got_ref[...].astype(jnp.float32)
    query = (base_ref[...].astype(jnp.float32) + delta).astype(jnp.bfloat16)
    scale = 1.0 / math.sqrt(size)
    for c in range(0, requests // CHUNK, 2):
        jobs = [(c + n, h) for n in range(2) for h in range(heads)]
        scores = []
        for n, h in jobs:
            rows = slice(n * CHUNK, (n + 1) * CHUNK)
            q = jnp.concatenate(
                [
                    query[rows, (h * group + g) * size : (h * group + g + 1) * size]
                    for g in range(group)
                ],
                axis=0,
            )
            k = k_ref[:, rows, h * size : (h + 1) * size].reshape(wide, size)
            scores.append(
                lax.dot_general(q, k, (((1,), (1,)), ((), ())), preferred_element_type=jnp.float32)
            )
        done = []
        for (n, h), score in zip(jobs, scores):
            rows = slice(n * CHUNK, (n + 1) * CHUNK)
            use = same & (valid_ref[n : n + 1, :] > 0.0)
            masked = jnp.where(use, score * scale, -jnp.inf)
            weights = jnp.exp(masked - jnp.max(masked, axis=-1, keepdims=True))
            total = jnp.sum(weights, axis=-1, keepdims=True)
            v = v_ref[:, rows, h * size : (h + 1) * size].reshape(wide, size)
            weighted = jnp.dot(weights.astype(jnp.bfloat16), v, preferred_element_type=jnp.float32)
            done.append((weighted * (1.0 / total)).astype(jnp.bfloat16))
        for (n, h), part in zip(jobs, done):
            rows = slice(n * CHUNK, (n + 1) * CHUNK)
            for g in range(group):
                out_ref[rows, (h * group + g) * size : (h * group + g + 1) * size] = part[
                    g * CHUNK : (g + 1) * CHUNK
                ]


def on_device(
    images,
    key_projection,
    value_projection,
    key_norm_gain,
    hidden,
    shared_query_base,
    adapter_down_matrix,
    adapter_up_matrix,
    tenant_adapter_index,
    used_tile_count,
):
    requests, half_model = hidden.shape
    size = key_norm_gain.shape[0]
    rank, width_query = adapter_up_matrix.shape[1:]
    here, tokens, width = images.shape
    banks = lax.axis_size("aa")
    side = math.isqrt(banks)
    assert side * side == banks and width_query == half_model
    held = side // 2 * SLOTS
    half = rank // 2
    both = ("aa", "ba")
    spot = range(side)
    lines = [[2 * (y * side + x) for y in spot] for x in spot]
    lines += [[2 * (y * side + x) + 1 for x in spot] for y in spot]
    beside = [
        (line[i] | 1, line[i ^ 1])
        for line in lines
        for i in spot
        if (line[i] // 2 // side + line[i] // 2 % side) % 2 == line[i] % 2
    ]
    swap = [(0, 1), (1, 0)]
    core = lax.axis_index("ba")
    bank = lax.axis_index("aa")
    column, line = bank % side, bank // side
    position = jnp.where(core == 0, line, column)
    flag = core.astype(jnp.int32).reshape(1)
    owned = (column + line) % 2 == core
    at = jnp.stack([core, position % 2, owned]).astype(jnp.int32)

    down, up = adapter_down_matrix[0].T, adapter_up_matrix[0]
    next_down = lax.ppermute(down, both, beside)
    next_up = lax.ppermute(up, both, beside)
    far_hidden = lax.ppermute(hidden, "ba", swap)
    slot = call(
        functools.partial(slot_kernel, side),
        [at, tenant_adapter_index.reshape(1, requests)],
        jax.ShapeDtypeStruct((8, requests), jnp.int32),
        2 * 10**10,
    )
    packed = call(
        functools.partial(pack_kernel, side),
        [at, slot, hidden, far_hidden, down, up, next_down, next_up],
        jax.ShapeDtypeStruct((side, 2 * held + 3 * half, half_model), jnp.bfloat16),
        4 * side * held * requests * half_model,
    )
    received = lax.all_to_all(packed, both, 0, 0, axis_index_groups=lines, tiled=True)

    x = images.transpose(1, 0, 2).reshape(tokens * here, width)
    keys, values = project(x, key_projection, value_projection, key_norm_gain[None, :])
    kept = lax.dynamic_slice_in_dim(shared_query_base, core * here, here, 0)
    sent = lax.dynamic_slice_in_dim(shared_query_base, (1 - core) * here, here, 0)
    got = lax.ppermute(sent, "ba", swap)
    base = jnp.concatenate(
        [jnp.where(core == 0, kept, got), jnp.where(core == 0, got, kept)], axis=1
    )
    tile = jnp.arange(tokens, dtype=jnp.int32) // TILE_TOKENS
    valid = tile[None, :, None] < used_tile_count.reshape(here // CHUNK, 1, CHUNK)
    valid = valid.astype(jnp.float32).reshape(here // CHUNK, tokens * CHUNK)
    received, keys, values, base, valid = lax.optimization_barrier(
        (received, keys, values, base, valid)
    )

    bank_rows = lax.ppermute(received[:, 2 * held :], "ba", swap)
    raised = call(
        functools.partial(raise_kernel, side, rank),
        [received, bank_rows],
        jax.ShapeDtypeStruct((side, held, width_query), jnp.bfloat16),
        6 * side * held * side * half * half_model,
    )
    back = lax.all_to_all(raised, both, 0, 0, axis_index_groups=lines, tiled=True)
    back = back.reshape(side * held, width_query)
    part = jax.ShapeDtypeStruct((here, width_query), jnp.bfloat16)
    mine, other = pl.pallas_call(
        unpack_kernel,
        out_shape=[part, part],
        in_specs=[SMEM, VMEM, VMEM],
        out_specs=[VMEM, VMEM],
        scratch_shapes=[pltpu.VMEM((requests, width_query), jnp.float32)],
        compiler_params=pltpu.CompilerParams(vmem_limit_bytes=24 * 2**20),
        cost_estimate=pl.CostEstimate(
            flops=2 * side * held * requests * width_query,
            bytes_accessed=4 * back.size,
            transcendentals=0,
        ),
        name="unpack",
    )(flag, slot, back)
    rest = lax.ppermute(other, "ba", swap)
    kvw = key_projection.shape[1]
    return call(
        functools.partial(attend_kernel, tokens, kvw // size, width_query // kvw, size),
        [
            mine,
            rest,
            base,
            keys.reshape(tokens, here, kvw),
            values.reshape(tokens, here, kvw),
            valid,
        ],
        jax.ShapeDtypeStruct((here, width_query), jnp.bfloat16),
        4 * here * width_query * tokens * CHUNK,
    )


def solution(mesh):
    placed = (
        P(("ga", "aa", "ba"), None, None),
        P(),
        P(),
        P(),
        P(("ga", "aa"), "ba"),
        P(("ga", "aa"), "ba"),
        P("aa", None, None),
        P("aa", None, None),
        P(("ga", "aa"), None),
        P(("ga", "aa", "ba")),
    )
    return jax.shard_map(
        on_device,
        mesh=mesh,
        in_specs=placed,
        out_specs=P(("ga", "aa", "ba"), None),
        check_vma=False,
    )
```

```python
import functools
import math

import jax
import jax.numpy as jnp
from jax import lax
from jax.experimental import pallas as pl
from jax.experimental.pallas import tpu as pltpu
from jax.sharding import PartitionSpec as P

TILE_TOKENS = 3
CHUNK = 16
FULL = 67043328
SLOTS = 4
VMEM = pl.BlockSpec(memory_space=pltpu.VMEM)
SMEM = pl.BlockSpec(memory_space=pltpu.SMEM)
HBM = pl.BlockSpec(memory_space=pltpu.HBM)


def call(kernel, ins, out, flops, limit=24):
    outs = jax.tree.leaves(out)
    specs = [SMEM if v.ndim == 1 else VMEM for v in ins]
    return pl.pallas_call(
        kernel,
        out_shape=out,
        in_specs=specs,
        out_specs=jax.tree.map(lambda _: VMEM, out),
        compiler_params=pltpu.CompilerParams(vmem_limit_bytes=limit * 2**20),
        cost_estimate=pl.CostEstimate(
            flops=flops,
            bytes_accessed=sum(v.size * v.dtype.itemsize for v in [*ins, *outs]),
            transcendentals=0,
        ),
    )(*ins)


def project_kernel(heads, size, x_ref, wk_ref, wv_ref, gain_ref, keys_ref, values_ref):
    x = x_ref[...]
    raw = jnp.dot(x, wk_ref[...], preferred_element_type=jnp.float32)
    for h in range(heads):
        part = raw[:, h * size : (h + 1) * size]
        scale = lax.rsqrt(jnp.mean(part * part, axis=-1, keepdims=True) + 1e-06)
        keys_ref[:, h * size : (h + 1) * size] = (part * scale * gain_ref[...]).astype(jnp.bfloat16)
    values_ref[...] = jnp.dot(x, wv_ref[...], preferred_element_type=jnp.float32).astype(jnp.bfloat16)


def project(x, wk, wv, gain):
    rows, width = x.shape
    kvw = wk.shape[1]
    size = gain.shape[1]
    tile = rows // 6 if rows % 96 == 0 else rows
    whole = lambda i: (0, 0)
    return pl.pallas_call(
        functools.partial(project_kernel, kvw // size, size),
        grid=(rows // tile,),
        in_specs=[
            pl.BlockSpec((tile, width), lambda i: (i, 0)),
            pl.BlockSpec((width, kvw), whole),
            pl.BlockSpec((width, kvw), whole),
            pl.BlockSpec((1, size), whole),
        ],
        out_specs=[pl.BlockSpec((tile, kvw), lambda i: (i, 0))] * 2,
        out_shape=[jax.ShapeDtypeStruct((rows, kvw), jnp.bfloat16)] * 2,
        compiler_params=pltpu.CompilerParams(vmem_limit_bytes=40 * 2**20),
        cost_estimate=pl.CostEstimate(
            flops=4 * rows * width * kvw,
            bytes_accessed=2 * (rows * width + 2 * width * kvw + 2 * rows * kvw),
            transcendentals=0,
        ),
        name="project",
    )(x, wk, wv, gain)


def placing_of(slot, slots):
    row = lax.broadcasted_iota(jnp.int32, (slots, slot.shape[1]), 0)
    return jnp.where(row == slot, 1.0, 0.0).astype(jnp.bfloat16)


def slot_kernel(side, at_ref, names_ref, slot_ref):
    requests = names_ref.shape[1]
    held = side // 2 * SLOTS
    core = at_ref[0]
    names = names_ref[...]
    across = jnp.broadcast_to(names.astype(jnp.float32), (requests, requests))
    down = jnp.transpose(across)
    low = lax.broadcasted_iota(jnp.int32, (requests, requests), 0)
    high = lax.broadcasted_iota(jnp.int32, (requests, requests), 1)
    earlier = jnp.where((across == down) & (low < high), 1.0, 0.0)
    rank = jnp.sum(earlier, axis=0, keepdims=True).astype(jnp.int32)
    column = names % side
    line = names // side
    peer = jnp.where(core == 0, line, column)
    which = jnp.where(core == 0, column, line) // 2
    slot = jnp.where((column + line) % 2 == 1 - core, peer * held + which * SLOTS + rank, -1)
    slot_ref[...] = jnp.broadcast_to(slot, slot_ref.shape)


def pack_kernel(
    side, at_ref, slot_ref, mine_ref, other_ref, down_ref, up_ref, next_down_ref, next_up_ref, out_ref,
    placed, piece, sems
):
    held = side // 2 * SLOTS
    core, odd, owned = at_ref[0], at_ref[1], at_ref[2]
    width = other_ref.shape[1]
    half = down_ref.shape[0] // 2
    moves = []

    def send(source, low, high, group):
        for p in range(side):
            move = pltpu.make_async_copy(
                source(p), out_ref.at[p, low:high], sems.at[group * side + p]
            )
            move.start()
            moves.append(move)

    def cut(down, up, low):
        rows = slice(low * half, (low + 1) * half)
        left, right = down[rows, :width], down[rows, width:]
        piece[:half] = jnp.where(core == 0, right, left)
        piece[half : 2 * half] = jnp.where(core == 0, left, right)
        piece[2 * half :] = up[rows]

    for own, (down, up) in ((1, (down_ref, up_ref)), (0, (next_down_ref, next_up_ref))):
        for low in (0, 1):

            @pl.when((owned == own) & (odd == low))
            def _():
                cut(down, up, low)

    send(lambda p: piece, 2 * held, 2 * held + 3 * half, 2)
    placing = placing_of(slot_ref[:1], side * held)
    for n, source in enumerate((mine_ref, other_ref)):
        placed[n] = jnp.dot(placing, source[...], preferred_element_type=jnp.float32).astype(
            jnp.bfloat16
        )
        send(lambda p: placed.at[n, p * held : (p + 1) * held], n * held, (n + 1) * held, n)
    for move in moves:
        move.wait()


def raise_kernel(side, rank, rows_ref, bank_ref, out_ref):
    held = side // 2 * SLOTS
    half = rank // 2
    width = rows_ref.shape[2]
    mine = rows_ref[:, :held].reshape(side * held, width)
    other = rows_ref[:, held : 2 * held].reshape(side * held, width)
    first = bank_ref[:, :half].reshape(side * half, width)
    second = bank_ref[:, half : 2 * half].reshape(side * half, width)
    up = bank_ref[:, 2 * half :].reshape(side * half, width)
    contract = (((1,), (1,)), ((), ()))
    low = lax.dot_general(mine, first, contract, preferred_element_type=jnp.float32)
    low = low + lax.dot_general(other, second, contract, preferred_element_type=jnp.float32)
    row = lax.broadcasted_iota(jnp.int32, low.shape, 0)
    col = lax.broadcasted_iota(jnp.int32, low.shape, 1)
    low = jnp.where((row // SLOTS) % (side // 2) == col // rank, low, 0.0).astype(jnp.bfloat16)
    raised = jnp.dot(low, up, preferred_element_type=jnp.float32).astype(jnp.bfloat16)
    out_ref[...] = raised.reshape(side, held, width)


def unpack_kernel(core_ref, slot_ref, back_ref, mine_ref, other_ref, whole):
    requests = slot_ref.shape[1]
    here = mine_ref.shape[0]
    core = core_ref[0]
    slots = back_ref.shape[0]
    row = lax.broadcasted_iota(jnp.int32, (slots, requests), 0)
    placing = jnp.where(row == slot_ref[:1], 1.0, 0.0).astype(jnp.bfloat16)
    whole[...] = lax.dot_general(
        placing, back_ref[...], (((0,), (0,)), ((), ())), preferred_element_type=jnp.float32
    )
    mine_ref[...] = whole[pl.ds(pl.multiple_of(core * here, here), here)].astype(jnp.bfloat16)
    other_ref[...] = whole[pl.ds(pl.multiple_of((1 - core) * here, here), here)].astype(
        jnp.bfloat16
    )


def attend_kernel(
    tokens, heads, group, size, mine_ref, got_ref, base_ref, k_ref, v_ref, valid_ref, out_ref
):
    requests = base_ref.shape[0]
    wide = tokens * CHUNK
    row = lax.broadcasted_iota(jnp.int32, (group * CHUNK, wide), 0)
    col = lax.broadcasted_iota(jnp.int32, (group * CHUNK, wide), 1)
    same = (row % CHUNK) == (col % CHUNK)
    delta = mine_ref[...].astype(jnp.float32) + got_ref[...].astype(jnp.float32)
    query = (base_ref[...].astype(jnp.float32) + delta).astype(jnp.bfloat16)
    scale = 1.0 / math.sqrt(size)
    for c in range(0, requests // CHUNK, 2):
        jobs = [(c + n, h) for n in range(2) for h in range(heads)]
        scores = []
        for n, h in jobs:
            rows = slice(n * CHUNK, (n + 1) * CHUNK)
            q = jnp.concatenate(
                [
                    query[rows, (h * group + g) * size : (h * group + g + 1) * size]
                    for g in range(group)
                ],
                axis=0,
            )
            k = k_ref[:, rows, h * size : (h + 1) * size].reshape(wide, size)
            scores.append(
                lax.dot_general(q, k, (((1,), (1,)), ((), ())), preferred_element_type=jnp.float32)
            )
        done = []
        for (n, h), score in zip(jobs, scores):
            rows = slice(n * CHUNK, (n + 1) * CHUNK)
            use = same & (valid_ref[n : n + 1, :] > 0.0)
            masked = jnp.where(use, score * scale, -jnp.inf)
            weights = jnp.exp(masked - jnp.max(masked, axis=-1, keepdims=True))
            total = jnp.sum(weights, axis=-1, keepdims=True)
            v = v_ref[:, rows, h * size : (h + 1) * size].reshape(wide, size)
            weighted = jnp.dot(weights.astype(jnp.bfloat16), v, preferred_element_type=jnp.float32)
            done.append((weighted * (1.0 / total)).astype(jnp.bfloat16))
        for (n, h), part in zip(jobs, done):
            rows = slice(n * CHUNK, (n + 1) * CHUNK)
            for g in range(group):
                out_ref[rows, (h * group + g) * size : (h * group + g + 1) * size] = part[
                    g * CHUNK : (g + 1) * CHUNK
                ]


def on_device(
    images,
    key_projection,
    value_projection,
    key_norm_gain,
    hidden,
    shared_query_base,
    adapter_down_matrix,
    adapter_up_matrix,
    tenant_adapter_index,
    used_tile_count,
):
    requests, half_model = hidden.shape
    size = key_norm_gain.shape[0]
    rank, width_query = adapter_up_matrix.shape[1:]
    here, tokens, width = images.shape
    banks = lax.axis_size("aa")
    side = math.isqrt(banks)
    assert side * side == banks and width_query == half_model
    held = side // 2 * SLOTS
    half = rank // 2
    both = ("aa", "ba")
    spot = range(side)
    lines = [[2 * (y * side + x) for y in spot] for x in spot]
    lines += [[2 * (y * side + x) + 1 for x in spot] for y in spot]
    beside = [
        (line[i] | 1, line[i ^ 1])
        for line in lines
        for i in spot
        if (line[i] // 2 // side + line[i] // 2 % side) % 2 == line[i] % 2
    ]
    swap = [(0, 1), (1, 0)]
    core = lax.axis_index("ba")
    bank = lax.axis_index("aa")
    column, line = bank % side, bank // side
    position = jnp.where(core == 0, line, column)
    flag = core.astype(jnp.int32).reshape(1)
    owned = (column + line) % 2 == core
    at = jnp.stack([core, position % 2, owned]).astype(jnp.int32)

    down, up = adapter_down_matrix[0].T, adapter_up_matrix[0]
    next_down = lax.ppermute(down, both, beside)
    next_up = lax.ppermute(up, both, beside)
    far_hidden = lax.ppermute(hidden, "ba", swap)
    slot = call(
        functools.partial(slot_kernel, side),
        [at, tenant_adapter_index.reshape(1, requests)],
        jax.ShapeDtypeStruct((8, requests), jnp.int32),
        2 * 10**10,
    )
    packed = pl.pallas_call(
        functools.partial(pack_kernel, side),
        out_shape=jax.ShapeDtypeStruct((side, 2 * held + 3 * half, half_model), jnp.bfloat16),
        in_specs=[SMEM] + [VMEM] * 7,
        out_specs=HBM,
        scratch_shapes=[
            pltpu.VMEM((2, side * held, half_model), jnp.bfloat16),
            pltpu.VMEM((3 * half, half_model), jnp.bfloat16),
            pltpu.SemaphoreType.DMA((3 * side,)),
        ],
        compiler_params=pltpu.CompilerParams(vmem_limit_bytes=FULL - 12288 * 2**10),
        cost_estimate=pl.CostEstimate(
            flops=4 * side * held * requests * half_model,
            bytes_accessed=4 * hidden.size,
            transcendentals=0,
        ),
        name="pack",
    )(at, slot, hidden, far_hidden, down, up, next_down, next_up)
    received = lax.all_to_all(packed, both, 0, 0, axis_index_groups=lines, tiled=True)

    x = images.transpose(1, 0, 2).reshape(tokens * here, width)
    keys, values = project(x, key_projection, value_projection, key_norm_gain[None, :])
    kept = lax.dynamic_slice_in_dim(shared_query_base, core * here, here, 0)
    sent = lax.dynamic_slice_in_dim(shared_query_base, (1 - core) * here, here, 0)
    got = lax.ppermute(sent, "ba", swap)
    base = jnp.concatenate(
        [jnp.where(core == 0, kept, got), jnp.where(core == 0, got, kept)], axis=1
    )
    tile = jnp.arange(tokens, dtype=jnp.int32) // TILE_TOKENS
    valid = tile[None, :, None] < used_tile_count.reshape(here // CHUNK, 1, CHUNK)
    valid = valid.astype(jnp.float32).reshape(here // CHUNK, tokens * CHUNK)
    received, keys, values, base, valid = lax.optimization_barrier(
        (received, keys, values, base, valid)
    )

    bank_rows = lax.ppermute(received[:, 2 * held :], "ba", swap)
    raised = call(
        functools.partial(raise_kernel, side, rank),
        [received, bank_rows],
        jax.ShapeDtypeStruct((side, held, width_query), jnp.bfloat16),
        6 * side * held * side * half * half_model,
    )
    back = lax.all_to_all(raised, both, 0, 0, axis_index_groups=lines, tiled=True)
    back = back.reshape(side * held, width_query)
    part = jax.ShapeDtypeStruct((here, width_query), jnp.bfloat16)
    mine, other = pl.pallas_call(
        unpack_kernel,
        out_shape=[part, part],
        in_specs=[SMEM, VMEM, VMEM],
        out_specs=[VMEM, VMEM],
        scratch_shapes=[pltpu.VMEM((requests, width_query), jnp.float32)],
        compiler_params=pltpu.CompilerParams(vmem_limit_bytes=24 * 2**20),
        cost_estimate=pl.CostEstimate(
            flops=2 * side * held * requests * width_query,
            bytes_accessed=4 * back.size,
            transcendentals=0,
        ),
        name="unpack",
    )(flag, slot, back)
    rest = lax.ppermute(other, "ba", swap)
    kvw = key_projection.shape[1]
    return call(
        functools.partial(attend_kernel, tokens, kvw // size, width_query // kvw, size),
        [
            mine,
            rest,
            base,
            keys.reshape(tokens, here, kvw),
            values.reshape(tokens, here, kvw),
            valid,
        ],
        jax.ShapeDtypeStruct((here, width_query), jnp.bfloat16),
        4 * here * width_query * tokens * CHUNK,
    )


def solution(mesh):
    placed = (
        P(("ga", "aa", "ba"), None, None),
        P(),
        P(),
        P(),
        P(("ga", "aa"), "ba"),
        P(("ga", "aa"), "ba"),
        P("aa", None, None),
        P("aa", None, None),
        P(("ga", "aa"), None),
        P(("ga", "aa", "ba")),
    )
    return jax.shard_map(
        on_device,
        mesh=mesh,
        in_specs=placed,
        out_specs=P(("ga", "aa", "ba"), None),
        check_vma=False,
    )
```
